32 devices in a mesh: groups: 2 (over y), seq: 4 (over z), head: 4 (over x, core).
Axes of the slice: x: 2, y: 2, z: 4, core: 2. Of those that a mesh axis runs over, the one named last changes fastest.
Arguments:
- queries: bfloat16 [2048, 8192], P(('groups', 'seq'), 'head'), parts along dimension 0, may hold values from -16 to 16
- keys: bfloat16 [2048, 1024], P(('groups', 'seq'), 'head'), parts along dimension 0, may hold values from -16 to 16
- values: bfloat16 [2048, 1024], P(('groups', 'seq'), 'head'), parts along dimension 0, may hold values from -6 to 6
- prompt_len: int32 [2], P('groups'), parts along dimension 0, may hold values from 256 to 1024
- page_dest: int32 [8, 2], P('groups'), parts along dimension 0, may hold values from 0 to 3, all different within a row; in each aligned block of 4 rows (0 to 3, 4 to 7, ...) at most 4 rows name the same one
Outputs:
- attended: bfloat16 [2048, 8192], P(('groups', 'seq'), 'head'), parts along dimension 0
- decode_page_cache: bfloat16 [32, 128, 2048], P(('groups', 'seq'), None, 'head'), parts along dimension 0
The draws below stay inside these ranges and needn't reach their ends.
There are 2 independent parts, one for each index of `groups`. The reference program is written for one: setup_inputs(seed, part) draws one part's arguments, and reference() takes and returns one part's arrays. A program takes and returns all parts, laid end to end along the dimension named above; each array names one. Nothing has to cross between parts.
Inputs may be any that keep to these rules, and one draw needn't show every extreme that they name: `page_dest`: row s names the decode devices of the 2 pages of tokens s * 256 to (s + 1) * 256 - 1, all different within a row; no device is named more than 4 times in all, and some device exactly 4 times.
All inputs are finite; a program needn't handle non-finite values.
Results may differ from the reference program's by a relative error of at most 0.005.
Values may be sent and summed in bfloat16 or wider, within the bound.
A program may use at most 64 MiB of HBM per device.

```python
import math
import jax
import jax.numpy as jnp
import numpy as np
from jax import lax

QUERY_HEADS = 64
KEY_VALUE_HEADS = 8
HEAD_SIZE = 128
PAGE_TOKENS = 128
QUERY_PER_KV = 8
PROMPT_TOKENS = 1024
PPD = 2
DEVICE_SLOTS = 4
PROMPT_PAGES = 8
N_SEQ = 4


def starting_rows(key, columns):
    return jnp.clip(jax.random.normal(jax.random.fold_in(key, 13), (PROMPT_TOKENS, columns), jnp.float32), -4.0, 4.0)


def draw_queries(key, part):
    sampled_inputs = starting_rows(jax.random.fold_in(key, 21), QUERY_HEADS * HEAD_SIZE)
    return sampled_inputs.astype(jnp.bfloat16)


def draw_keys(key, part):
    sampled_inputs = starting_rows(jax.random.fold_in(key, 22), KEY_VALUE_HEADS * HEAD_SIZE)
    return sampled_inputs.astype(jnp.bfloat16)


def steps_of(stream_key, shape, split, smallest, high):
    def one(position, parts):
        heights = jax.random.uniform(jax.random.fold_in(jax.random.fold_in(stream_key, 6), position), (parts,), jnp.float32, smallest / len(split), high / len(split))
        return jnp.repeat(jnp.exp(heights), shape[position] // parts).reshape((-1,) + (1,) * (len(shape) - position - 1))

    loudness = one(*split[0])
    for cut in split[1:]:
        loudness = loudness * one(*cut)
    return loudness


def deal_out(stream_key, own, number, rows, amount, top, most, slope):
    order = jax.random.permutation(stream_key, amount)
    packed, ordinary = portions_of(amount, rows * top, most, slope, True), portions_of(amount, rows * top, most, slope, False)
    places = jnp.arange(amount)

    def named(tallies, rotation):
        used = int((tallies > 0).sum())
        fixed = max(1, used // 4)
        passed = fixed + (places - fixed + rotation * (used - fixed)) % max(1, amount - fixed)
        return jnp.zeros((amount,), jnp.int32).at[order[jnp.where(places < fixed, places, passed)]].set(jnp.asarray(tallies, jnp.int32))

    tallies = jnp.where(number % 4 == 0, named(packed, number // 4), named(ordinary, number - number // 4 - 1))
    mixed = jax.random.permutation(jax.random.fold_in(own, 3), amount)
    source_of, receiver = mixed[0:amount // 2 * 2:2], mixed[1:amount // 2 * 2:2]
    room = jnp.minimum(tallies[source_of] - 1, most - tallies[receiver]) // 2
    room = jnp.where((source_of == order[0]) | (receiver == order[0]) | (tallies[receiver] == 0), 0, jnp.maximum(room, 0))
    passed = jax.random.randint(jax.random.fold_in(own, 4), (amount // 2,), 0, 1 << 20) % (room + 1)
    tallies = tallies.at[source_of].add(-passed).at[receiver].add(passed)
    members = jnp.searchsorted(jnp.cumsum(tallies), jnp.arange(rows * top), side="right").astype(jnp.int32)
    listing = members.reshape(top, rows).T
    listing = listing[jax.random.permutation(jax.random.fold_in(own, 1), rows)]
    rotation = jax.random.randint(jax.random.fold_in(own, 2), (rows, 1), 0, top)
    return jnp.take_along_axis(listing, (jnp.arange(top)[None, :] + rotation) % top, axis=1)


def portions_of(amount, total, limit, slope, full):
    portions = [(1 << 20) // math.isqrt(grade ** slope) + 1 for grade in range(1, amount + 1)]
    largest = limit if full else min(limit, max(-(-total // amount), total * portions[0] // sum(portions)))
    least = 1 if total - largest >= amount - 1 else 0
    counts, spare = [largest] + [least] * (amount - 1), total - largest - least * (amount - 1)
    while spare > 0:
        candidates = [i for i in range(1, amount) if counts[i] < largest] or [i for i in range(1, amount) if counts[i] < limit]
        pool, remaining = sum([portions[i] for i in candidates]), spare
        for i in candidates:
            addition = min(limit - counts[i], max(1, remaining * portions[i] // pool), spare)
            counts[i] = counts[i] + addition
            spare = spare - addition
    return np.array(counts)


def gaussian(stream_key, dims, width, reach, pieces=(), kind=jnp.bfloat16):
    drawn = jax.random.normal(stream_key, dims, jnp.float32) * width
    if len(pieces) > 0:
        drawn = steps_of(stream_key, dims, pieces, -0.22, 0.18) * drawn
    return jnp.clip(drawn, min=-reach, max=reach).astype(kind)


def setup_inputs(seed: int = 0, part: int = 0) -> dict:
    splits = jax.random.split(jax.random.key(seed), 6)
    part_splits = jax.random.split(jax.random.fold_in(splits[5], part), 6)
    queries = draw_queries(jax.random.fold_in(jax.random.fold_in(splits[5], part), 71), part)
    keys = draw_keys(jax.random.fold_in(jax.random.fold_in(splits[5], part), 71), part)
    values = gaussian(part_splits[2], (PROMPT_TOKENS, KEY_VALUE_HEADS * HEAD_SIZE), 1.0, 6.0, ((0, 4), (1, 4)))
    prompt_len = jax.random.randint(part_splits[3], (1,), PROMPT_TOKENS // 4, PROMPT_TOKENS + 1).astype(jnp.int32)
    page_dest_keys = jax.random.split(jax.random.fold_in(part_splits[4], 1), N_SEQ // N_SEQ)
    page_dest_turns = jax.random.permutation(jax.random.fold_in(part_splits[4], 3), N_SEQ // N_SEQ)
    page_dest = jax.vmap(lambda own, number: deal_out(jax.random.fold_in(part_splits[4], 2), own, number, N_SEQ, N_SEQ, PPD, DEVICE_SLOTS, 2))(page_dest_keys, page_dest_turns).reshape((N_SEQ, PPD))
    return {"queries": queries, "keys": keys, "values": values, "prompt_len": prompt_len, "page_dest": page_dest}


NEG_FILL = -1e+30

def reference(queries, keys, values, prompt_len, page_dest):
    prompt_end = prompt_len[0]
    score_scale = 1.0 / math.sqrt(HEAD_SIZE)
    rows_in_block = math.gcd(PROMPT_TOKENS, 256)
    blocks = PROMPT_TOKENS // rows_in_block
    positions = jnp.arange(PROMPT_TOKENS, dtype=jnp.int32)
    key_live = positions < prompt_end
    key_head_rows = keys.reshape(PROMPT_TOKENS, KEY_VALUE_HEADS, HEAD_SIZE).transpose(1, 0, 2).astype(jnp.float32)
    value_head_rows = values.reshape(PROMPT_TOKENS, KEY_VALUE_HEADS, HEAD_SIZE).transpose(1, 0, 2).astype(jnp.float32)

    def query_block(number):
        first_row = (number * rows_in_block).astype(jnp.int32)
        query_block_rows = lax.dynamic_slice_in_dim(queries, first_row, rows_in_block, 0)
        query_block_rows = query_block_rows.reshape(rows_in_block, KEY_VALUE_HEADS, QUERY_PER_KV, HEAD_SIZE).transpose(1, 2, 0, 3).astype(jnp.float32)
        query_pos = first_row + jnp.arange(rows_in_block, dtype=jnp.int32)
        allowed = (positions[None, :] <= query_pos[:, None]) & key_live[None, :]
        query_live = query_pos < prompt_end

        def one_head(head_items):
            head_rows, head_keys, head_values = head_items
            scores = jnp.einsum('grd,pd->grp', head_rows, head_keys) * score_scale
            scores = jnp.where(allowed[None], scores, NEG_FILL)
            row_max = lax.optimization_barrier(jnp.max(scores, axis=-1, keepdims=True))
            weights = jnp.where(allowed[None], jnp.exp(scores - row_max), 0.0)
            denominator = lax.optimization_barrier(jnp.sum(weights, axis=-1))
            rounded = lax.optimization_barrier(weights.astype(jnp.bfloat16)).astype(jnp.float32)
            weighted = jnp.einsum('grp,pd->grd', rounded, head_values)
            safe_total = jnp.where(query_live[None, :], denominator, 1.0)
            return jnp.where(query_live[None, :, None], weighted / safe_total[..., None], 0.0)
        result = lax.map(one_head, (query_block_rows, key_head_rows, value_head_rows))
        return result.transpose(2, 0, 1, 3).reshape(rows_in_block, QUERY_HEADS * HEAD_SIZE).astype(jnp.bfloat16)
    attended = lax.map(query_block, jnp.arange(blocks, dtype=jnp.int32)).reshape(PROMPT_TOKENS, QUERY_HEADS * HEAD_SIZE)
    flat_dest = page_dest.reshape(-1).astype(jnp.int32)
    page_order = jnp.arange(PROMPT_PAGES, dtype=jnp.int32)
    same_dest = flat_dest[:, None] == flat_dest[None, :]
    dest_rank = lax.optimization_barrier(jnp.sum(same_dest & (page_order[None, :] < page_order[:, None]), axis=1)).astype(jnp.int32)
    target_slot_index = (flat_dest * DEVICE_SLOTS + dest_rank).astype(jnp.int32)
    token_present = key_live[:, None]
    retained_keys = jnp.where(token_present, keys, jnp.zeros((), jnp.bfloat16)).reshape(PROMPT_PAGES, PAGE_TOKENS, KEY_VALUE_HEADS, HEAD_SIZE)
    retained_values = jnp.where(token_present, values, jnp.zeros((), jnp.bfloat16)).reshape(PROMPT_PAGES, PAGE_TOKENS, KEY_VALUE_HEADS, HEAD_SIZE)
    page_content = jnp.stack((retained_keys, retained_values), axis=3).reshape(PROMPT_PAGES, PAGE_TOKENS, 2 * KEY_VALUE_HEADS * HEAD_SIZE)
    decode_page_cache = jnp.zeros((N_SEQ * DEVICE_SLOTS, PAGE_TOKENS, 2 * KEY_VALUE_HEADS * HEAD_SIZE), jnp.bfloat16).at[target_slot_index].set(page_content)
    return (attended, decode_page_cache)
```

```python
import functools
import math

import jax
import jax.numpy as jnp
from jax import lax
from jax.experimental import pallas as pl
from jax.experimental.pallas import tpu as pltpu
from jax.sharding import PartitionSpec as P

HEAD = 128
PAGE = 128
NEG = -1e30
MESH = pl.DeviceIdType.MESH


def kernel(
    n, kv_heads, group, slots,
    plen_ref, dest_ref, q_hbm, k_hbm, v_hbm,
    att_ref, cache_ref,
    q_ref, kv, m_ref, acc_ref, p_ref, slot_ref,
    q_sem, own_sem, up_send, down_send, recv_sem,
):
    me = lax.axis_index("seq")
    rows = q_ref.shape[0]
    chunks = 2 * kv_heads
    ppd = rows // PAGE
    coef = math.log2(math.e) / math.sqrt(HEAD)

    def own_copy(c):
        src = k_hbm if c % 2 == 0 else v_hbm
        return pltpu.make_async_copy(
            src.at[:, pl.ds((c // 2) * HEAD, HEAD)], kv.at[me, c], own_sem.at[c]
        )

    q_copy = pltpu.make_async_copy(q_hbm, q_ref, q_sem)
    for c in range(chunks):
        own_copy(c).start()
    q_copy.start()

    barrier = pltpu.get_barrier_semaphore()

    @pl.when(me > 0)
    def _():
        pl.semaphore_signal(barrier, inc=1, device_id={"seq": me - 1}, device_id_type=MESH)

    @pl.when(me < n - 1)
    def _():
        pl.semaphore_signal(barrier, inc=1, device_id={"seq": me + 1}, device_id_type=MESH)

    pl.semaphore_wait(barrier, jnp.minimum(me, 1) + jnp.minimum(n - 1 - me, 1))

    def up(blk, c):
        return pltpu.make_async_remote_copy(
            src_ref=kv.at[blk, c], dst_ref=kv.at[blk, c],
            send_sem=up_send.at[blk, c], recv_sem=recv_sem.at[blk, c],
            device_id={"seq": me + 1}, device_id_type=MESH,
        )

    def down(blk, c):
        return pltpu.make_async_remote_copy(
            src_ref=kv.at[blk, c], dst_ref=kv.at[blk, c],
            send_sem=down_send.at[blk, c], recv_sem=recv_sem.at[blk, c],
            device_id={"seq": me - 1}, device_id_type=MESH,
        )

    for c in range(chunks):
        own_copy(c).wait()

        @pl.when(me < n - 1)
        def _():
            up(me, c).start()

        @pl.when(me > 0)
        def _():
            down(me, c).start()

    end = plen_ref[0]

    def rank(page, seen):
        hit = dest_ref[page // ppd, page % ppd] == me
        slot_ref[page] = jnp.where(hit, seen, -1)
        return seen + jnp.where(hit, 1, 0)

    lax.fori_loop(0, n * ppd, rank, jnp.int32(0))
    cache_ref[...] = jnp.zeros_like(cache_ref)
    token = lax.broadcasted_iota(jnp.int32, (PAGE, HEAD), 0)

    def store_pages(blk, c):
        lane = pl.ds(c * HEAD, HEAD)
        for k in range(ppd):
            number = blk * ppd + k
            page = kv[blk, c, k * PAGE:(k + 1) * PAGE, :]
            for r in range(slots):
                limit = jnp.where(slot_ref[number] == r, end - number * PAGE, 0)
                cache_ref[r, :, lane] = jnp.where(token < limit, page, cache_ref[r, :, lane])

    q_copy.wait()

    def cols(h):
        return pl.ds(pl.multiple_of(h * HEAD, HEAD), HEAD)

    def scores(g, h, blk):
        q = q_ref[:, cols(h)]
        return lax.dot_general(
            q, kv[blk, 2 * g], (((1,), (1,)), ((), ())), preferred_element_type=jnp.float32
        )

    def weigh(p, g, blk):
        v = kv[blk, 2 * g + 1]
        v = jnp.concatenate([v, jnp.ones_like(v)], axis=1)
        return jnp.dot(p, v, preferred_element_type=jnp.float32)

    causal = lax.broadcasted_iota(jnp.int32, (rows, rows), 1) <= lax.broadcasted_iota(
        jnp.int32, (rows, rows), 0
    )

    def diagonal(g):
        @pl.loop(0, group, unroll=2)
        def _(i):
            h = g * group + i
            s = jnp.where(causal, scores(g, h, me), NEG)
            m = jnp.max(s, axis=1, keepdims=True)
            p = jnp.exp2((s - m) * coef)
            m_ref[h] = jnp.broadcast_to(m, (rows, HEAD))
            acc_ref[h] = weigh(p.astype(jnp.bfloat16), g, me)

    for g in range(kv_heads):
        diagonal(g)
    for c in range(chunks):
        store_pages(me, c)

    def pass_k(g, blk):
        @pl.loop(0, group, unroll=2)
        def _(i):
            h = g * group + i
            s = scores(g, h, blk)
            old = m_ref[h]
            new = jnp.maximum(old, jnp.max(s, axis=1, keepdims=True))
            p = jnp.exp2((s - jnp.concatenate([new] * (rows // HEAD), axis=1)) * coef)
            factor = jnp.exp2((old - new) * coef)
            m_ref[h] = new
            p_ref[i] = p.astype(jnp.bfloat16)
            acc_ref[h] = acc_ref[h] * jnp.concatenate([factor, factor], axis=1)

    def pass_v(g, blk):
        @pl.loop(0, group, unroll=2)
        def _(i):
            h = g * group + i
            acc_ref[h] = acc_ref[h] + weigh(p_ref[i], g, blk)

    def step(t, c):
        @pl.when(me >= t)
        def _():
            up(me - t, c).wait_recv()

            @pl.when(me < n - 1)
            def _():
                up(me - t, c).start()

        @pl.when(me + t < n)
        def _():
            down(me + t, c).wait_recv()

            @pl.when(me > 0)
            def _():
                down(me + t, c).start()

            store_pages(me + t, c)

        @pl.when(me >= t)
        def _():
            store_pages(me - t, c)
            if c % 2 == 0:
                pass_k(c // 2, me - t)
            else:
                pass_v(c // 2, me - t)

    @pl.loop(1, n)
    def _(t):
        for c in range(chunks):
            step(t, c)

    live = (
        me * rows + lax.broadcasted_iota(jnp.int32, (rows, HEAD), 0)
    ) < end

    @pl.loop(0, kv_heads * group, unroll=2)
    def _(h):
        out = jnp.where(live, acc_ref[h, :, :HEAD] / acc_ref[h, :, HEAD:], 0.0)
        att_ref[:, cols(h)] = out.astype(jnp.bfloat16)

    @pl.loop(0, n)
    def _(blk):
        @pl.loop(0, chunks)
        def _(c):
            @pl.when((blk <= me) & (me < n - 1))
            def _():
                up(blk, c).wait_send()

            @pl.when((blk >= me) & (me > 0))
            def _():
                down(blk, c).wait_send()


def local(n, queries, keys, values, prompt_len, page_dest):
    rows, width = queries.shape
    kv_heads = keys.shape[1] // HEAD
    heads = width // HEAD
    group = heads // kv_heads
    slots = 2 * page_dest.shape[1]
    chunks = 2 * kv_heads
    hbm = pl.BlockSpec(memory_space=pltpu.HBM)
    vmem = pl.BlockSpec(memory_space=pltpu.VMEM)
    smem = pl.BlockSpec(memory_space=pltpu.SMEM)
    return pl.pallas_call(
        functools.partial(kernel, n, kv_heads, group, slots),
        out_shape=(
            jax.ShapeDtypeStruct((rows, width), jnp.bfloat16),
            jax.ShapeDtypeStruct((slots, PAGE, chunks * HEAD), jnp.bfloat16),
        ),
        in_specs=[smem, smem, hbm, hbm, hbm],
        out_specs=(vmem, vmem),
        scratch_shapes=[
            pltpu.VMEM((rows, width), jnp.bfloat16),
            pltpu.VMEM((n, chunks, rows, HEAD), jnp.bfloat16),
            pltpu.VMEM((heads, rows, HEAD), jnp.float32),
            pltpu.VMEM((heads, rows, 2 * HEAD), jnp.float32),
            pltpu.VMEM((group, rows, rows), jnp.bfloat16),
            pltpu.SMEM((n * rows // PAGE,), jnp.int32),
            pltpu.SemaphoreType.DMA,
            pltpu.SemaphoreType.DMA((chunks,)),
            pltpu.SemaphoreType.DMA((n, chunks)),
            pltpu.SemaphoreType.DMA((n, chunks)),
            pltpu.SemaphoreType.DMA((n, chunks)),
        ],
        compiler_params=pltpu.CompilerParams(
            collective_id=0, has_side_effects=True, vmem_limit_bytes=48 * 1024 * 1024
        ),
    )(prompt_len, page_dest, queries, keys, values)


def solution(mesh):
    return jax.shard_map(
        functools.partial(local, mesh.shape["seq"]),
        mesh=mesh,
        in_specs=(
            P(("groups", "seq"), "head"),
            P(("groups", "seq"), "head"),
            P(("groups", "seq"), "head"),
            P("groups"),
            P("groups", None),
        ),
        out_specs=(P(("groups", "seq"), "head"), P(("groups", "seq"), None, "head")),
        check_vma=False,
    )
```

```python
import functools
import math

import jax
import jax.numpy as jnp
from jax import lax
from jax.experimental import pallas as pl
from jax.experimental.pallas import tpu as pltpu
from jax.sharding import PartitionSpec as P

HEAD = 128
PAGE = 128
NEG = -1e30
MESH = pl.DeviceIdType.MESH


def kernel(
    n, kv_heads, group, slots,
    plen_ref, dest_hbm, q_hbm, k_hbm, v_hbm,
    att_ref, cache_ref,
    q_ref, kv, m_ref, acc_ref, p_ref, slot_ref, dest_ref,
    q_sem, own_sem, up_send, down_send, recv_sem, dest_sem,
):
    me = lax.axis_index("seq")
    rows = q_ref.shape[0]
    chunks = 2 * kv_heads
    ppd = rows // PAGE
    coef = math.log2(math.e) / math.sqrt(HEAD)

    def own_copy(c):
        src = k_hbm if c % 2 == 0 else v_hbm
        return pltpu.make_async_copy(
            src.at[:, pl.ds((c // 2) * HEAD, HEAD)], kv.at[me, c], own_sem.at[c]
        )

    q_copy = pltpu.make_async_copy(q_hbm, q_ref, q_sem)
    for c in range(chunks):
        own_copy(c).start()
    q_copy.start()
    dest_copy = pltpu.make_async_copy(dest_hbm, dest_ref, dest_sem)
    dest_copy.start()

    barrier = pltpu.get_barrier_semaphore()

    @pl.when(me > 0)
    def _():
        pl.semaphore_signal(barrier, inc=1, device_id={"seq": me - 1}, device_id_type=MESH)

    @pl.when(me < n - 1)
    def _():
        pl.semaphore_signal(barrier, inc=1, device_id={"seq": me + 1}, device_id_type=MESH)

    pl.semaphore_wait(barrier, jnp.minimum(me, 1) + jnp.minimum(n - 1 - me, 1))

    def up(blk, c):
        return pltpu.make_async_remote_copy(
            src_ref=kv.at[blk, c], dst_ref=kv.at[blk, c],
            send_sem=up_send.at[blk, c], recv_sem=recv_sem.at[blk, c],
            device_id={"seq": me + 1}, device_id_type=MESH,
        )

    def down(blk, c):
        return pltpu.make_async_remote_copy(
            src_ref=kv.at[blk, c], dst_ref=kv.at[blk, c],
            send_sem=down_send.at[blk, c], recv_sem=recv_sem.at[blk, c],
            device_id={"seq": me - 1}, device_id_type=MESH,
        )

    for c in range(chunks):
        own_copy(c).wait()

        @pl.when(me < n - 1)
        def _():
            up(me, c).start()

        @pl.when(me > 0)
        def _():
            down(me, c).start()

    dest_copy.wait()
    end = plen_ref[0]
    live = (me * rows + lax.broadcasted_iota(jnp.int32, (rows, HEAD), 0)) < end

    def rank(page, seen):
        hit = dest_ref[page % ppd, page // ppd] == me
        slot_ref[page] = jnp.where(hit, seen, -1)
        return seen + jnp.where(hit, 1, 0)

    lax.fori_loop(0, n * ppd, rank, jnp.int32(0))
    cache_ref[...] = jnp.zeros_like(cache_ref)
    token = lax.broadcasted_iota(jnp.int32, (PAGE, HEAD), 0)

    def store_pages(blk, c):
        lane = pl.ds(c * HEAD, HEAD)
        for k in range(ppd):
            number = blk * ppd + k
            page = kv[blk, c, k * PAGE:(k + 1) * PAGE, :]
            for r in range(slots):
                limit = jnp.where(slot_ref[number] == r, end - number * PAGE, 0)
                cache_ref[r, :, lane] = jnp.where(token < limit, page, cache_ref[r, :, lane])

    q_copy.wait()

    def cols(h):
        return pl.ds(pl.multiple_of(h * HEAD, HEAD), HEAD)

    def scores(g, h, blk):
        q = q_ref[:, cols(h)]
        return lax.dot_general(
            q, kv[blk, 2 * g], (((1,), (1,)), ((), ())), preferred_element_type=jnp.float32
        )

    def weigh(p, g, blk):
        v = kv[blk, 2 * g + 1]
        v = jnp.concatenate([v, jnp.ones_like(v)], axis=1)
        return jnp.dot(p, v, preferred_element_type=jnp.float32)

    causal = lax.broadcasted_iota(jnp.int32, (rows, rows), 1) <= lax.broadcasted_iota(
        jnp.int32, (rows, rows), 0
    )

    def finish(h, total):
        out = jnp.where(live, total[:, :HEAD] / total[:, HEAD:], 0.0)
        att_ref[:, cols(h)] = out.astype(jnp.bfloat16)

    def diagonal(g):
        @pl.loop(0, group, unroll=2)
        def _(i):
            h = g * group + i
            s = jnp.where(causal, scores(g, h, me), NEG)
            m = jnp.max(s, axis=1, keepdims=True)
            p = jnp.exp2((s - m) * coef)
            m_ref[h] = jnp.broadcast_to(m, (rows, HEAD))
            acc_ref[h] = weigh(p.astype(jnp.bfloat16), g, me)

    for g in range(kv_heads):
        diagonal(g)

    @pl.when(me == 0)
    def _():
        @pl.loop(0, kv_heads * group)
        def _(h):
            finish(h, acc_ref[h])

    for c in range(chunks):
        store_pages(me, c)

    def pass_k(g, blk):
        @pl.loop(0, group, unroll=2)
        def _(i):
            h = g * group + i
            s = scores(g, h, blk)
            old = m_ref[h]
            new = jnp.maximum(old, jnp.max(s, axis=1, keepdims=True))
            p = jnp.exp2((s - jnp.concatenate([new] * (rows // HEAD), axis=1)) * coef)
            factor = jnp.exp2((old - new) * coef)
            m_ref[h] = new
            p_ref[i] = p.astype(jnp.bfloat16)
            acc_ref[h] = acc_ref[h] * jnp.concatenate([factor, factor], axis=1)

    def pass_v(g, blk, last):
        @pl.loop(0, group, unroll=2)
        def _(i):
            h = g * group + i
            total = acc_ref[h] + weigh(p_ref[i], g, blk)
            if last:
                finish(h, total)
            else:
                acc_ref[h] = total

    def step(t, c):
        @pl.when(me >= t)
        def _():
            up(me - t, c).wait_recv()

            @pl.when(me < n - 1)
            def _():
                up(me - t, c).start()

        @pl.when(me + t < n)
        def _():
            down(me + t, c).wait_recv()

            @pl.when(me > 0)
            def _():
                down(me + t, c).start()

            store_pages(me + t, c)

        @pl.when(me >= t)
        def _():
            store_pages(me - t, c)
            if c % 2 == 0:
                pass_k(c // 2, me - t)
            else:

                @pl.when(me > t)
                def _():
                    pass_v(c // 2, me - t, False)

                @pl.when(me == t)
                def _():
                    pass_v(c // 2, me - t, True)

    @pl.loop(1, n)
    def _(t):
        for c in range(chunks):
            step(t, c)

    @pl.loop(0, n)
    def _(blk):
        @pl.loop(0, chunks)
        def _(c):
            @pl.when((blk <= me) & (me < n - 1))
            def _():
                up(blk, c).wait_send()

            @pl.when((blk >= me) & (me > 0))
            def _():
                down(blk, c).wait_send()


def write_out(att_ref, cache_ref, att_hbm, cache_hbm, sem):
    att_copy = pltpu.make_async_copy(att_ref, att_hbm, sem.at[0])
    cache_copy = pltpu.make_async_copy(cache_ref, cache_hbm, sem.at[1])
    att_copy.start()
    cache_copy.start()
    att_copy.wait()
    cache_copy.wait()


def local(n, queries, keys, values, prompt_len, page_dest):
    rows, width = queries.shape
    kv_heads = keys.shape[1] // HEAD
    heads = width // HEAD
    group = heads // kv_heads
    slots = 2 * page_dest.shape[1]
    chunks = 2 * kv_heads
    hbm = pl.BlockSpec(memory_space=pltpu.HBM)
    smem = pl.BlockSpec(memory_space=pltpu.SMEM)
    vmem = pl.BlockSpec(memory_space=pltpu.VMEM)
    att, cache = pl.pallas_call(
        functools.partial(kernel, n, kv_heads, group, slots),
        out_shape=(
            jax.ShapeDtypeStruct((rows, width), jnp.bfloat16),
            jax.ShapeDtypeStruct((slots, PAGE, chunks * HEAD), jnp.bfloat16),
        ),
        in_specs=[smem] + [hbm] * 4,
        out_specs=(vmem, vmem),
        scratch_shapes=[
            pltpu.VMEM((rows, width), jnp.bfloat16),
            pltpu.VMEM((n, chunks, rows, HEAD), jnp.bfloat16),
            pltpu.VMEM((heads, rows, HEAD), jnp.float32),
            pltpu.VMEM((heads, rows, 2 * HEAD), jnp.float32),
            pltpu.VMEM((group, rows, rows), jnp.bfloat16),
            pltpu.SMEM((n * rows // PAGE,), jnp.int32),
            pltpu.SMEM(page_dest.shape[::-1], jnp.int32),
            pltpu.SemaphoreType.DMA,
            pltpu.SemaphoreType.DMA((chunks,)),
            pltpu.SemaphoreType.DMA((n, chunks)),
            pltpu.SemaphoreType.DMA((n, chunks)),
            pltpu.SemaphoreType.DMA((n, chunks)),
            pltpu.SemaphoreType.DMA,
        ],
        compiler_params=pltpu.CompilerParams(
            collective_id=0, has_side_effects=True, vmem_limit_bytes=48 * 1024 * 1024
        ),
    )(prompt_len, *(
        pltpu.with_memory_space_constraint(x, pltpu.HBM)
        for x in (page_dest.T, queries, keys, values)
    ))
    return pl.pallas_call(
        write_out,
        out_shape=(
            jax.ShapeDtypeStruct(att.shape, att.dtype),
            jax.ShapeDtypeStruct(cache.shape, cache.dtype),
        ),
        in_specs=[vmem, vmem],
        out_specs=(hbm, hbm),
        scratch_shapes=[pltpu.SemaphoreType.DMA((2,))],
        compiler_params=pltpu.CompilerParams(vmem_limit_bytes=8 * 1024 * 1024),
    )(att, cache)


def solution(mesh):
    return jax.shard_map(
        functools.partial(local, mesh.shape["seq"]),
        mesh=mesh,
        in_specs=(
            P(("groups", "seq"), "head"),
            P(("groups", "seq"), "head"),
            P(("groups", "seq"), "head"),
            P("groups"),
            P("groups", None),
        ),
        out_specs=(P(("groups", "seq"), "head"), P(("groups", "seq"), None, "head")),
        check_vma=False,
    )
```

```python
import functools
import math

import jax
import jax.numpy as jnp
from jax import lax
from jax.experimental import pallas as pl
from jax.experimental.pallas import tpu as pltpu
from jax.sharding import PartitionSpec as P

HEAD = 128
PAGE = 128
NEG = -1e30
MESH = pl.DeviceIdType.MESH


def kernel(
    n, kv_heads, group, slots,
    plen_ref, dest_hbm, q_hbm, k_hbm, v_hbm,
    att_ref, cache_ref,
    q_ref, kv, m_ref, l_ref, acc_ref, p_ref, slot_ref, dest_ref,
    q_sem, own_sem, up_send, down_send, recv_sem, dest_sem,
):
    me = lax.axis_index("seq")
    rows = q_ref.shape[0]
    chunks = 2 * kv_heads
    ppd = rows // PAGE
    coef = math.log2(math.e) / math.sqrt(HEAD)

    def own_copy(c):
        src = k_hbm if c % 2 == 0 else v_hbm
        return pltpu.make_async_copy(
            src.at[:, pl.ds((c // 2) * HEAD, HEAD)], kv.at[me, c], own_sem.at[c]
        )

    q_copy = pltpu.make_async_copy(q_hbm, q_ref, q_sem)
    for c in range(chunks):
        own_copy(c).start()
    dest_copy = pltpu.make_async_copy(dest_hbm, dest_ref, dest_sem)
    dest_copy.start()

    barrier = pltpu.get_barrier_semaphore()

    @pl.when(me > 0)
    def _():
        pl.semaphore_signal(barrier, inc=1, device_id={"seq": me - 1}, device_id_type=MESH)

    @pl.when(me < n - 1)
    def _():
        pl.semaphore_signal(barrier, inc=1, device_id={"seq": me + 1}, device_id_type=MESH)

    pl.semaphore_wait(barrier, jnp.minimum(me, 1) + jnp.minimum(n - 1 - me, 1))

    def up(blk, c):
        return pltpu.make_async_remote_copy(
            src_ref=kv.at[blk, c], dst_ref=kv.at[blk, c],
            send_sem=up_send.at[blk, c], recv_sem=recv_sem.at[blk, c],
            device_id={"seq": me + 1}, device_id_type=MESH,
        )

    def down(blk, c):
        return pltpu.make_async_remote_copy(
            src_ref=kv.at[blk, c], dst_ref=kv.at[blk, c],
            send_sem=down_send.at[blk, c], recv_sem=recv_sem.at[blk, c],
            device_id={"seq": me - 1}, device_id_type=MESH,
        )

    for c in range(chunks):
        own_copy(c).wait()

        @pl.when(me < n - 1)
        def _():
            up(me, c).start()

        @pl.when(me > 0)
        def _():
            down(me, c).start()

    q_copy.start()
    dest_copy.wait()
    end = plen_ref[0]
    live = (me * rows + lax.broadcasted_iota(jnp.int32, (rows, HEAD), 0)) < end

    def rank(page, seen):
        hit = dest_ref[page % ppd, page // ppd] == me
        slot_ref[page] = jnp.where(hit, seen, -1)
        return seen + jnp.where(hit, 1, 0)

    lax.fori_loop(0, n * ppd, rank, jnp.int32(0))
    cache_ref[...] = jnp.zeros_like(cache_ref)
    token = lax.broadcasted_iota(jnp.int32, (PAGE, HEAD), 0)

    def store_pages(blk, c):
        lane = pl.ds(c * HEAD, HEAD)
        for k in range(ppd):
            number = blk * ppd + k
            page = kv[blk, c, k * PAGE:(k + 1) * PAGE, :]
            for r in range(slots):
                limit = jnp.where(slot_ref[number] == r, end - number * PAGE, 0)
                cache_ref[r, :, lane] = jnp.where(token < limit, page, cache_ref[r, :, lane])

    q_copy.wait()

    def cols(h):
        return pl.ds(pl.multiple_of(h * HEAD, HEAD), HEAD)

    def scores(g, h, blk):
        q = q_ref[:, cols(h)]
        return lax.dot_general(
            q, kv[blk, 2 * g], (((1,), (1,)), ((), ())), preferred_element_type=jnp.float32
        )

    def weigh(p, g, blk):
        return jnp.dot(p, kv[blk, 2 * g + 1], preferred_element_type=jnp.float32)

    def total(p):
        return jnp.dot(p, jnp.ones((rows, HEAD), jnp.bfloat16), preferred_element_type=jnp.float32)

    causal = lax.broadcasted_iota(jnp.int32, (rows, rows), 1) <= lax.broadcasted_iota(
        jnp.int32, (rows, rows), 0
    )

    def invert(h):
        l_ref[h] = jnp.where(live, 1.0 / l_ref[h], 0.0)

    def finish(h, value):
        att_ref[:, cols(h)] = (value * l_ref[h]).astype(jnp.bfloat16)

    def diagonal(g):
        @pl.loop(0, group, unroll=2)
        def _(i):
            h = g * group + i
            s = jnp.where(causal, scores(g, h, me), NEG)
            m = jnp.max(s, axis=1, keepdims=True)
            p = jnp.exp2((s - m) * coef).astype(jnp.bfloat16)
            m_ref[h] = jnp.broadcast_to(m, (rows, HEAD))
            l_ref[h] = total(p)
            acc_ref[h] = weigh(p, g, me)

    for g in range(kv_heads):
        diagonal(g)

    @pl.when(me == 0)
    def _():
        @pl.loop(0, kv_heads * group)
        def _(h):
            invert(h)
            finish(h, acc_ref[h])

    for c in range(chunks):
        store_pages(me, c)

    def pass_k(g, blk):
        @pl.loop(0, group, unroll=2)
        def _(i):
            h = g * group + i
            s = scores(g, h, blk)
            old = m_ref[h]
            new = jnp.maximum(old, jnp.max(s, axis=1, keepdims=True))
            p = jnp.exp2((s - jnp.concatenate([new] * (rows // HEAD), axis=1)) * coef)
            p = p.astype(jnp.bfloat16)
            factor = jnp.exp2((old - new) * coef)
            m_ref[h] = new
            p_ref[i] = p
            l_ref[h] = l_ref[h] * factor + total(p)
            acc_ref[h] = acc_ref[h] * factor

    def pass_v(g, blk, last):
        @pl.loop(0, group, unroll=2)
        def _(i):
            h = g * group + i
            value = acc_ref[h] + weigh(p_ref[i], g, blk)
            if last:
                finish(h, value)
            else:
                acc_ref[h] = value

    def step(t, c):
        @pl.when(me >= t)
        def _():
            up(me - t, c).wait_recv()

            @pl.when(me < n - 1)
            def _():
                up(me - t, c).start()

        @pl.when(me + t < n)
        def _():
            down(me + t, c).wait_recv()

            @pl.when(me > 0)
            def _():
                down(me + t, c).start()

            store_pages(me + t, c)

        @pl.when(me >= t)
        def _():
            g = c // 2
            if c % 2 == 0:
                pass_k(g, me - t)

                @pl.when(me == t)
                def _():
                    @pl.loop(0, group)
                    def _(i):
                        invert(g * group + i)
            else:
                @pl.when(me > t)
                def _():
                    pass_v(g, me - t, False)

                @pl.when(me == t)
                def _():
                    pass_v(g, me - t, True)
            store_pages(me - t, c)

    @pl.loop(1, n)
    def _(t):
        for c in range(chunks):
            step(t, c)

    @pl.loop(0, n)
    def _(blk):
        @pl.loop(0, chunks)
        def _(c):
            @pl.when((blk <= me) & (me < n - 1))
            def _():
                up(blk, c).wait_send()

            @pl.when((blk >= me) & (me > 0))
            def _():
                down(blk, c).wait_send()


def write_out(att_ref, cache_ref, att_hbm, cache_hbm, sem):
    att_copy = pltpu.make_async_copy(att_ref, att_hbm, sem.at[0])
    cache_copy = pltpu.make_async_copy(cache_ref, cache_hbm, sem.at[1])
    att_copy.start()
    cache_copy.start()
    att_copy.wait()
    cache_copy.wait()


def local(n, queries, keys, values, prompt_len, page_dest):
    rows, width = queries.shape
    kv_heads = keys.shape[1] // HEAD
    heads = width // HEAD
    group = heads // kv_heads
    slots = 2 * page_dest.shape[1]
    chunks = 2 * kv_heads
    hbm = pl.BlockSpec(memory_space=pltpu.HBM)
    vmem = pl.BlockSpec(memory_space=pltpu.VMEM)
    att, cache = pl.pallas_call(
        functools.partial(kernel, n, kv_heads, group, slots),
        out_shape=(
            jax.ShapeDtypeStruct((rows, width), jnp.bfloat16),
            jax.ShapeDtypeStruct((slots, PAGE, chunks * HEAD), jnp.bfloat16),
        ),
        in_specs=[pl.BlockSpec(memory_space=pltpu.SMEM)] + [hbm] * 4,
        out_specs=(vmem, vmem),
        scratch_shapes=[
            pltpu.VMEM((rows, width), jnp.bfloat16),
            pltpu.VMEM((n, chunks, rows, HEAD), jnp.bfloat16),
            pltpu.VMEM((heads, rows, HEAD), jnp.float32),
            pltpu.VMEM((heads, rows, HEAD), jnp.float32),
            pltpu.VMEM((heads, rows, HEAD), jnp.float32),
            pltpu.VMEM((group, rows, rows), jnp.bfloat16),
            pltpu.SMEM((n * rows // PAGE,), jnp.int32),
            pltpu.SMEM(page_dest.shape[::-1], jnp.int32),
            pltpu.SemaphoreType.DMA,
            pltpu.SemaphoreType.DMA((chunks,)),
            pltpu.SemaphoreType.DMA((n, chunks)),
            pltpu.SemaphoreType.DMA((n, chunks)),
            pltpu.SemaphoreType.DMA((n, chunks)),
            pltpu.SemaphoreType.DMA,
        ],
        compiler_params=pltpu.CompilerParams(
            collective_id=0, has_side_effects=True, vmem_limit_bytes=48 * 1024 * 1024
        ),
    )(prompt_len, *(
        pltpu.with_memory_space_constraint(x, pltpu.HBM)
        for x in (page_dest.T, queries, keys, values)
    ))
    return pl.pallas_call(
        write_out,
        out_shape=(
            jax.ShapeDtypeStruct(att.shape, att.dtype),
            jax.ShapeDtypeStruct(cache.shape, cache.dtype),
        ),
        in_specs=[vmem, vmem],
        out_specs=(hbm, hbm),
        scratch_shapes=[pltpu.SemaphoreType.DMA((2,))],
        compiler_params=pltpu.CompilerParams(vmem_limit_bytes=8 * 1024 * 1024),
    )(att, cache)


def solution(mesh):
    return jax.shard_map(
        functools.partial(local, mesh.shape["seq"]),
        mesh=mesh,
        in_specs=(
            P(("groups", "seq"), "head"),
            P(("groups", "seq"), "head"),
            P(("groups", "seq"), "head"),
            P("groups"),
            P("groups", None),
        ),
        out_specs=(P(("groups", "seq"), "head"), P(("groups", "seq"), None, "head")),
        check_vma=False,
    )
```

```python
import functools
import math

import jax
import jax.numpy as jnp
from jax import lax
from jax.experimental import pallas as pl
from jax.experimental.pallas import tpu as pltpu
from jax.sharding import PartitionSpec as P

HEAD = 128
PAGE = 128
NEG = -1e30
MESH = pl.DeviceIdType.MESH


def kernel(
    n, kv_heads, group, slots,
    plen_ref, dest_hbm, q_hbm, k_hbm, v_hbm,
    att_ref, cache_ref,
    q_ref, kv, m_ref, acc_ref, p_ref, slot_ref, dest_ref,
    q_sem, own_sem, up_send, down_send, recv_sem, dest_sem,
):
    me = lax.axis_index("seq")
    rows = q_ref.shape[0]
    chunks = 2 * kv_heads
    ppd = rows // PAGE
    coef = math.log2(math.e) / math.sqrt(HEAD)

    def own_copy(c):
        src = k_hbm if c % 2 == 0 else v_hbm
        return pltpu.make_async_copy(
            src.at[:, pl.ds((c // 2) * HEAD, HEAD)], kv.at[me, c], own_sem.at[c]
        )

    q_copy = pltpu.make_async_copy(q_hbm, q_ref, q_sem)
    for c in range(chunks):
        own_copy(c).start()
    dest_copy = pltpu.make_async_copy(dest_hbm, dest_ref, dest_sem)
    dest_copy.start()

    barrier = pltpu.get_barrier_semaphore()

    @pl.when(me > 0)
    def _():
        pl.semaphore_signal(barrier, inc=1, device_id={"seq": me - 1}, device_id_type=MESH)

    @pl.when(me < n - 1)
    def _():
        pl.semaphore_signal(barrier, inc=1, device_id={"seq": me + 1}, device_id_type=MESH)

    pl.semaphore_wait(barrier, jnp.minimum(me, 1) + jnp.minimum(n - 1 - me, 1))

    def up(blk, c):
        return pltpu.make_async_remote_copy(
            src_ref=kv.at[blk, c], dst_ref=kv.at[blk, c],
            send_sem=up_send.at[blk, c], recv_sem=recv_sem.at[blk, c],
            device_id={"seq": me + 1}, device_id_type=MESH,
        )

    def down(blk, c):
        return pltpu.make_async_remote_copy(
            src_ref=kv.at[blk, c], dst_ref=kv.at[blk, c],
            send_sem=down_send.at[blk, c], recv_sem=recv_sem.at[blk, c],
            device_id={"seq": me - 1}, device_id_type=MESH,
        )

    for c in range(chunks):
        own_copy(c).wait()

        @pl.when(me < n - 1)
        def _():
            up(me, c).start()

        @pl.when(me > 0)
        def _():
            down(me, c).start()

    q_copy.start()
    dest_copy.wait()
    end = plen_ref[0]
    live = (me * rows + lax.broadcasted_iota(jnp.int32, (rows, HEAD), 0)) < end

    def rank(page, seen):
        hit = dest_ref[page % ppd, page // ppd] == me
        slot_ref[page] = jnp.where(hit, seen, -1)
        return seen + jnp.where(hit, 1, 0)

    lax.fori_loop(0, n * ppd, rank, jnp.int32(0))
    cache_ref[...] = jnp.zeros_like(cache_ref)
    token = lax.broadcasted_iota(jnp.int32, (PAGE, HEAD), 0)

    def store_pages(blk, c):
        lane = pl.ds(c * HEAD, HEAD)
        for k in range(ppd):
            number = blk * ppd + k
            page = kv[blk, c, k * PAGE:(k + 1) * PAGE, :]
            for r in range(slots):
                limit = jnp.where(slot_ref[number] == r, end - number * PAGE, 0)
                cache_ref[r, :, lane] = jnp.where(token < limit, page, cache_ref[r, :, lane])

    q_copy.wait()

    def cols(h):
        return pl.ds(pl.multiple_of(h * HEAD, HEAD), HEAD)

    def scores(g, h, blk):
        q = q_ref[:, cols(h)]
        return lax.dot_general(
            q, kv[blk, 2 * g], (((1,), (1,)), ((), ())), preferred_element_type=jnp.float32
        )

    def weigh(p, g, blk):
        v = kv[blk, 2 * g + 1]
        v = jnp.concatenate([v, jnp.ones_like(v)], axis=1)
        return jnp.dot(p, v, preferred_element_type=jnp.float32)

    causal = lax.broadcasted_iota(jnp.int32, (rows, rows), 1) <= lax.broadcasted_iota(
        jnp.int32, (rows, rows), 0
    )

    def finish(h, total):
        out = jnp.where(live, total[:, :HEAD] / total[:, HEAD:], 0.0)
        att_ref[:, cols(h)] = out.astype(jnp.bfloat16)

    def diagonal(g):
        @pl.loop(0, group, unroll=2)
        def _(i):
            h = g * group + i
            s = jnp.where(causal, scores(g, h, me), NEG)
            m = jnp.max(s, axis=1, keepdims=True)
            p = jnp.exp2((s - m) * coef)
            m_ref[h] = jnp.broadcast_to(m, (rows, HEAD))
            acc_ref[h] = weigh(p.astype(jnp.bfloat16), g, me)

    for g in range(kv_heads):
        diagonal(g)

    @pl.when(me == 0)
    def _():
        @pl.loop(0, kv_heads * group)
        def _(h):
            finish(h, acc_ref[h])

    for c in range(chunks):
        store_pages(me, c)

    def pass_k(g, blk):
        @pl.loop(0, group, unroll=2)
        def _(i):
            h = g * group + i
            s = scores(g, h, blk)
            old = m_ref[h]
            new = jnp.maximum(old, jnp.max(s, axis=1, keepdims=True))
            p = jnp.exp2((s - jnp.concatenate([new] * (rows // HEAD), axis=1)) * coef)
            factor = jnp.exp2((old - new) * coef)
            m_ref[h] = new
            p_ref[i] = p.astype(jnp.bfloat16)
            acc_ref[h] = acc_ref[h] * jnp.concatenate([factor, factor], axis=1)

    def pass_v(g, blk, last):
        @pl.loop(0, group, unroll=4)
        def _(i):
            h = g * group + i
            total = acc_ref[h] + weigh(p_ref[i], g, blk)
            if last:
                finish(h, total)
            else:
                acc_ref[h] = total

    def step(t, c):
        @pl.when(me >= t)
        def _():
            up(me - t, c).wait_recv()

            @pl.when(me < n - 1)
            def _():
                up(me - t, c).start()

        @pl.when(me + t < n)
        def _():
            down(me + t, c).wait_recv()

            @pl.when(me > 0)
            def _():
                down(me + t, c).start()

            store_pages(me + t, c)

        @pl.when(me >= t)
        def _():
            if c % 2 == 0:
                store_pages(me - t, c)
                pass_k(c // 2, me - t)
            else:

                @pl.when(me > t)
                def _():
                    pass_v(c // 2, me - t, False)

                @pl.when(me == t)
                def _():
                    pass_v(c // 2, me - t, True)
                store_pages(me - t, c)

    @pl.loop(1, n)
    def _(t):
        for c in range(chunks):
            step(t, c)

    @pl.loop(0, n)
    def _(blk):
        @pl.loop(0, chunks)
        def _(c):
            @pl.when((blk <= me) & (me < n - 1))
            def _():
                up(blk, c).wait_send()

            @pl.when((blk >= me) & (me > 0))
            def _():
                down(blk, c).wait_send()


def write_out(att_ref, cache_ref, att_hbm, cache_hbm, sem):
    att_copy = pltpu.make_async_copy(att_ref, att_hbm, sem.at[0])
    cache_copy = pltpu.make_async_copy(cache_ref, cache_hbm, sem.at[1])
    att_copy.start()
    cache_copy.start()
    att_copy.wait()
    cache_copy.wait()


def local(n, queries, keys, values, prompt_len, page_dest):
    rows, width = queries.shape
    kv_heads = keys.shape[1] // HEAD
    heads = width // HEAD
    group = heads // kv_heads
    slots = 2 * page_dest.shape[1]
    chunks = 2 * kv_heads
    hbm = pl.BlockSpec(memory_space=pltpu.HBM)
    smem = pl.BlockSpec(memory_space=pltpu.SMEM)
    vmem = pl.BlockSpec(memory_space=pltpu.VMEM)
    att, cache = pl.pallas_call(
        functools.partial(kernel, n, kv_heads, group, slots),
        out_shape=(
            jax.ShapeDtypeStruct((rows, width), jnp.bfloat16),
            jax.ShapeDtypeStruct((slots, PAGE, chunks * HEAD), jnp.bfloat16),
        ),
        in_specs=[smem] + [hbm] * 4,
        out_specs=(vmem, vmem),
        scratch_shapes=[
            pltpu.VMEM((rows, width), jnp.bfloat16),
            pltpu.VMEM((n, chunks, rows, HEAD), jnp.bfloat16),
            pltpu.VMEM((heads, rows, HEAD), jnp.float32),
            pltpu.VMEM((heads, rows, 2 * HEAD), jnp.float32),
            pltpu.VMEM((group, rows, rows), jnp.bfloat16),
            pltpu.SMEM((n * rows // PAGE,), jnp.int32),
            pltpu.SMEM(page_dest.shape[::-1], jnp.int32),
            pltpu.SemaphoreType.DMA,
            pltpu.SemaphoreType.DMA((chunks,)),
            pltpu.SemaphoreType.DMA((n, chunks)),
            pltpu.SemaphoreType.DMA((n, chunks)),
            pltpu.SemaphoreType.DMA((n, chunks)),
            pltpu.SemaphoreType.DMA,
        ],
        compiler_params=pltpu.CompilerParams(
            collective_id=0, has_side_effects=True, vmem_limit_bytes=48 * 1024 * 1024
        ),
    )(prompt_len, *(
        pltpu.with_memory_space_constraint(x, pltpu.HBM)
        for x in (page_dest.T, queries, keys, values)
    ))
    return pl.pallas_call(
        write_out,
        out_shape=(
            jax.ShapeDtypeStruct(att.shape, att.dtype),
            jax.ShapeDtypeStruct(cache.shape, cache.dtype),
        ),
        in_specs=[vmem, vmem],
        out_specs=(hbm, hbm),
        scratch_shapes=[pltpu.SemaphoreType.DMA((2,))],
        compiler_params=pltpu.CompilerParams(vmem_limit_bytes=8 * 1024 * 1024),
    )(att, cache)


def solution(mesh):
    return jax.shard_map(
        functools.partial(local, mesh.shape["seq"]),
        mesh=mesh,
        in_specs=(
            P(("groups", "seq"), "head"),
            P(("groups", "seq"), "head"),
            P(("groups", "seq"), "head"),
            P("groups"),
            P("groups", None),
        ),
        out_specs=(P(("groups", "seq"), "head"), P(("groups", "seq"), None, "head")),
        check_vma=False,
    )
```
